16 devices in a mesh: dp: 2 (over z), ep: 8 (over y, x, core).
Axes of the slice: x: 2, y: 2, z: 2, core: 2. Of those that a mesh axis runs over, the one named last changes fastest.
Arguments:
- hidden: bfloat16 [16384, 768], P(('dp', 'ep'))
- route_idx: int32 [16384, 1], P(('dp', 'ep'))
- gates: bfloat16 [16384, 1], P(('dp', 'ep'))
- grad_out: bfloat16 [16384, 768], P(('dp', 'ep'))
- w_up: bfloat16 [8, 768, 3072], P('ep')
- w_lin: bfloat16 [8, 768, 3072], P('ep')
- w_down: bfloat16 [8, 3072, 768], P('ep')
- ws_up: bfloat16 [768, 3072], P(None, 'ep')
- ws_lin: bfloat16 [768, 3072], P(None, 'ep')
- ws_down: bfloat16 [3072, 768], P('ep')
Outputs:
- output 1: bfloat16 [16384, 768], P(('dp', 'ep'))
- output 2: bfloat16 [16384, 768], P(('dp', 'ep'))
- output 3: float32 [8, 768, 3072], P('ep')
- output 4: float32 [8, 768, 3072], P('ep')
- output 5: float32 [8, 3072, 768], P('ep')
- output 6: float32 [768, 3072], P(None, 'ep')
- output 7: float32 [768, 3072], P(None, 'ep')
- output 8: float32 [3072, 768], P('ep')
All inputs are finite; a program needn't handle non-finite values.
Results may differ from the reference program's by a relative error of at most 0.001.
Values are sent between devices in bfloat16 or wider.
A program may use at most 1 GiB of HBM per device.

```python
import jax
import jax.numpy as jnp
from jax import lax

D = 768
FF = 3072
FS = 3072
EXPERTS = 8
TOP = 1
DP = 2
EP = 8
TOK = 1024
HOT = 0


def draw_routing(rng_key):
    devices_all = DP * EP
    key_base, key_hot, key_count, key_full = jax.random.split(rng_key, 4)
    base_perm = jax.vmap(lambda sub_key: jax.random.permutation(sub_key, TOK))(jax.random.split(key_base, devices_all))
    hot_perm = jax.vmap(lambda sub_key: jax.random.permutation(sub_key, TOK))(jax.random.split(key_hot, devices_all))
    hot_count = jax.random.randint(key_count, (devices_all,), TOK // 8, TOK + 1)
    full_device = jax.random.randint(key_full, (), 0, devices_all)
    hot_count = jnp.where(jnp.arange(devices_all) == full_device, TOK, hot_count)
    is_hot = (hot_perm < hot_count[:, None]).astype(jnp.int32)
    base_slot = base_perm % (EXPERTS - 1)
    slot_ids = jnp.arange(TOP)
    others = 1 + (base_slot[:, :, None] + slot_ids[None, None, :] - is_hot[:, :, None]) % (EXPERTS - 1)
    route_all = jnp.where((is_hot[:, :, None] == 1) & (slot_ids[None, None, :] == 0), HOT, others)
    return route_all.reshape(devices_all * TOK, TOP).astype(jnp.int32)


def setup_inputs(seed: int = 0) -> dict:
    key_list = jax.random.split(jax.random.key(seed), 11)
    tokens_all = DP * EP * TOK
    hidden = jax.random.normal(key_list[0], (tokens_all, D), jnp.float32).astype(jnp.bfloat16)
    route_idx = draw_routing(key_list[1])
    gate_hot = jax.random.uniform(key_list[2], (tokens_all, TOP), jnp.float32, 0.6, 1.0)
    gate_rest = jax.random.uniform(key_list[3], (tokens_all, TOP), jnp.float32, 0.2, 1.0) * TOP ** -0.5
    gates = jnp.where(route_idx == HOT, gate_hot, gate_rest).astype(jnp.bfloat16)
    grad_out = jax.random.normal(key_list[4], (tokens_all, D), jnp.float32).astype(jnp.bfloat16)
    w_up = (jax.random.normal(key_list[5], (EXPERTS, D, FF), jnp.float32) * D ** -0.5).astype(jnp.bfloat16)
    w_lin = (jax.random.normal(key_list[6], (EXPERTS, D, FF), jnp.float32) * D ** -0.5).astype(jnp.bfloat16)
    w_down = (jax.random.normal(key_list[7], (EXPERTS, FF, D), jnp.float32) * FF ** -0.5).astype(jnp.bfloat16)
    ws_up = (jax.random.normal(key_list[8], (D, FS), jnp.float32) * D ** -0.5).astype(jnp.bfloat16)
    ws_lin = (jax.random.normal(key_list[9], (D, FS), jnp.float32) * D ** -0.5).astype(jnp.bfloat16)
    ws_down = (jax.random.normal(key_list[10], (FS, D), jnp.float32) * FS ** -0.5).astype(jnp.bfloat16)
    return {'hidden': hidden, 'route_idx': route_idx, 'gates': gates, 'grad_out': grad_out, 'w_up': w_up, 'w_lin': w_lin, 'w_down': w_down, 'ws_up': ws_up, 'ws_lin': ws_lin, 'ws_down': ws_down}


def expert_pass(tok_x, coeffs, tok_dy, w_up_e, w_lin_e, w_down_e):
    pre_up = jnp.dot(tok_x, w_up_e, preferred_element_type=jnp.float32)
    pre_lin = jnp.dot(tok_x, w_lin_e, preferred_element_type=jnp.float32)
    sig_up = jax.nn.sigmoid(pre_up)
    act_bf = (pre_up * sig_up * pre_lin).astype(jnp.bfloat16)
    out_bf = jnp.dot(act_bf, w_down_e, preferred_element_type=jnp.float32).astype(jnp.bfloat16)
    y_part = coeffs[:, None] * out_bf.astype(jnp.float32)
    d_rows = (coeffs[:, None] * tok_dy.astype(jnp.float32)).astype(jnp.bfloat16)
    d_act = jnp.dot(d_rows, w_down_e.T, preferred_element_type=jnp.float32)
    d_up = (d_act * pre_lin * sig_up * (1.0 + pre_up * (1.0 - sig_up))).astype(jnp.bfloat16)
    d_lin = (d_act * pre_up * sig_up).astype(jnp.bfloat16)
    g_down = jnp.dot(act_bf.T, d_rows, preferred_element_type=jnp.float32)
    g_up = jnp.dot(tok_x.T, d_up, preferred_element_type=jnp.float32)
    g_lin = jnp.dot(tok_x.T, d_lin, preferred_element_type=jnp.float32)
    dx_part = (jnp.dot(d_up, w_up_e.T, preferred_element_type=jnp.float32) + jnp.dot(d_lin, w_lin_e.T, preferred_element_type=jnp.float32)).astype(jnp.bfloat16)
    return y_part, dx_part, g_up, g_lin, g_down


def reference(hidden, route_idx, gates, grad_out, w_up, w_lin, w_down, ws_up, ws_lin, ws_down):
    cap_rows = TOP * ((TOK + EXPERTS - 2) // (EXPERTS - 1))
    span_rows = DP * EP * cap_rows
    gate_f = gates.astype(jnp.float32)
    hot_coef = jnp.sum(jnp.where(route_idx == HOT, gate_f, 0.0), axis=1)
    y_hot, dx_hot, h_up, h_lin, h_down = expert_pass(hidden, hot_coef, grad_out, w_up[HOT], w_lin[HOT], w_down[HOT])
    flat_ids = route_idx.reshape(-1)
    flat_gate = gate_f.reshape(-1)
    counts = jax.ops.segment_sum(jnp.ones_like(flat_ids), flat_ids, num_segments=EXPERTS)
    starts = jnp.cumsum(counts) - counts
    sort_order = jnp.concatenate([jnp.argsort(flat_ids, stable=True).astype(jnp.int32), jnp.zeros((span_rows,), jnp.int32)])

    def one_expert(acc_pair, expert):
        y_acc, dx_acc = acc_pair
        slot_src = lax.dynamic_slice(sort_order, (starts[expert],), (span_rows,))
        is_valid = jnp.arange(span_rows) < counts[expert]
        tok_ids = slot_src // TOP
        coeffs = jnp.where(is_valid, flat_gate[slot_src], 0.0)
        y_part, dx_part, g_up, g_lin, g_down = expert_pass(hidden[tok_ids], coeffs, grad_out[tok_ids], w_up[expert], w_lin[expert], w_down[expert])
        y_acc = y_acc.at[tok_ids].add(y_part)
        dx_acc = dx_acc.at[tok_ids].add(dx_part.astype(jnp.float32))
        return (y_acc, dx_acc), (g_up, g_lin, g_down)

    acc_pair, grad_stack = lax.scan(one_expert, (y_hot, dx_hot.astype(jnp.float32)), jnp.arange(1, EXPERTS))
    y_acc, dx_acc = acc_pair
    dw_up = jnp.concatenate([h_up[None], grad_stack[0]], axis=0)
    dw_lin = jnp.concatenate([h_lin[None], grad_stack[1]], axis=0)
    dw_down = jnp.concatenate([h_down[None], grad_stack[2]], axis=0)
    shared_up = jnp.dot(hidden, ws_up, preferred_element_type=jnp.float32)
    shared_lin = jnp.dot(hidden, ws_lin, preferred_element_type=jnp.float32)
    shared_sig = jax.nn.sigmoid(shared_up)
    shared_act = (shared_up * shared_sig * shared_lin).astype(jnp.bfloat16)
    shared_y = jnp.dot(shared_act, ws_down, preferred_element_type=jnp.float32)
    shared_dact = jnp.dot(grad_out, ws_down.T, preferred_element_type=jnp.float32)
    shared_dup = (shared_dact * shared_lin * shared_sig * (1.0 + shared_up * (1.0 - shared_sig))).astype(jnp.bfloat16)
    shared_dlin = (shared_dact * shared_up * shared_sig).astype(jnp.bfloat16)
    dws_down = jnp.dot(shared_act.T, grad_out, preferred_element_type=jnp.float32)
    dws_up = jnp.dot(hidden.T, shared_dup, preferred_element_type=jnp.float32)
    dws_lin = jnp.dot(hidden.T, shared_dlin, preferred_element_type=jnp.float32)
    shared_dx = jnp.dot(shared_dup, ws_up.T, preferred_element_type=jnp.float32) + jnp.dot(shared_dlin, ws_lin.T, preferred_element_type=jnp.float32)
    y_tok = (y_acc + shared_y).astype(jnp.bfloat16)
    d_hidden = (dx_acc + shared_dx).astype(jnp.bfloat16)
    return (y_tok, d_hidden, dw_up, dw_lin, dw_down, dws_up, dws_lin, dws_down)
```

```python
import functools

import jax
import jax.numpy as jnp
from jax import lax
from jax.experimental import pallas as pl
from jax.experimental.pallas import tpu as pltpu
from jax.sharding import PartitionSpec as P


HOT = 0
F32 = jnp.float32
BF16 = jnp.bfloat16
BIT = {'c': 1, 'x': 2, 'y': 4}


def mm(a, b, ca, cb):
    return lax.dot_general(a, b, (((ca,), (cb,)), ((), ())), preferred_element_type=F32)


def expert_tile(outer_rows, x_ref, d_ref, up_ref, lin_ref, dn_ref, *rest):
    row, col = pl.program_id(0), pl.program_id(1)
    if outer_rows:
        act_ref, du_ref, dl_ref, out_ref, dx_ref, out_acc, dx_acc = rest
    else:
        act_ref, du_ref, dl_ref = rest[-3:]
    up = mm(x_ref[...], up_ref[...], 1, 0)
    lin = mm(x_ref[...], lin_ref[...], 1, 0)
    d_act = mm(d_ref[...], dn_ref[...], 1, 1)
    sig = jax.nn.sigmoid(up)
    silu = up * sig
    act = (silu * lin).astype(BF16)
    d_up = (d_act * lin * sig * (1.0 + up * (1.0 - sig))).astype(BF16)
    d_lin = (d_act * silu).astype(BF16)
    act_ref[...] = act
    du_ref[...] = d_up
    dl_ref[...] = d_lin
    if outer_rows:
        out_part = mm(act, dn_ref[...], 1, 0)
        dx_part = mm(d_up, up_ref[...], 1, 1) + mm(d_lin, lin_ref[...], 1, 1)

        @pl.when(col == 0)
        def _():
            out_acc[...] = out_part
            dx_acc[...] = dx_part

        @pl.when(col > 0)
        def _():
            out_acc[...] += out_part
            dx_acc[...] += dx_part

        @pl.when(col == pl.num_programs(1) - 1)
        def _():
            out_ref[...] = out_acc[...].astype(out_ref.dtype)
            dx_ref[...] = dx_acc[...].astype(dx_ref.dtype)


def expert_call(x, d, up_w, lin_w, dn_w, out_type, tile, total_rows, saved=None):
    rows, width = x.shape
    ff = up_w.shape[1]
    ft = 512
    first = saved is None
    offset = 0 if first else rows // tile
    wide = pl.BlockSpec((tile, ft), lambda r, c: (r + offset, c))
    thin = pl.BlockSpec((tile, width), lambda r, c: (r, 0))
    in_specs = [thin, thin, pl.BlockSpec((width, ft), lambda r, c: (0, c)), pl.BlockSpec((width, ft), lambda r, c: (0, c)), pl.BlockSpec((ft, width), lambda r, c: (c, 0))]
    out_shape = [jax.ShapeDtypeStruct((total_rows, ff), BF16)] * 3
    out_specs = [wide] * 3
    scratch, alias, extra = [], {}, ()
    if first:
        out_shape += [jax.ShapeDtypeStruct((rows, width), out_type)] * 2
        out_specs += [thin] * 2
        scratch = [pltpu.VMEM((tile, width), F32)] * 2
    else:
        extra = saved
        in_specs += [pl.BlockSpec(memory_space=pl.ANY)] * 3
        alias = {5: 0, 6: 1, 7: 2}
    flops = 2 * rows * width * ff * (6 if first else 3)
    return pl.pallas_call(
        functools.partial(expert_tile, first),
        grid=(rows // tile, ff // ft),
        in_specs=in_specs,
        out_specs=out_specs,
        out_shape=out_shape,
        scratch_shapes=scratch,
        input_output_aliases=alias,
        cost_estimate=pl.CostEstimate(flops=flops, bytes_accessed=6 * rows * ff, transcendentals=rows * ff),
        compiler_params=pltpu.CompilerParams(dimension_semantics=('arbitrary', 'arbitrary'), vmem_limit_bytes=48 * 1024 * 1024),
    )(x, d, up_w, lin_w, dn_w, *extra)


MESH = pl.DeviceIdType.MESH
PIECES = (('up', 'x'), ('lin', 'y'), ('dna', 'x'), ('dnb', 'y'))


def weights_kernel(part, wsu, wsl, wsd, wu, wl, wd, su, sl, sd, hu, hl, hd, small_a, small_b, big_a, big_b, load_sem, store_sem, far_send, far_recv, ag_send, ag_recv, hot_send, hot_recv):
    rank = lax.axis_index('ep')
    chip, core = rank // 2, rank % 2
    half, zh = 4 * part, wsd.shape[1] // 2
    xbit, ybit = chip % 2, chip // 2
    x_chip = chip + 1 - 2 * xbit
    y_chip = chip + 2 - 4 * ybit
    xy_chip = 3 - chip

    def region(refs, name, slot):
        at = pl.ds(pl.multiple_of(slot * part, 128), part)
        if name == 'up':
            return refs[0].at[:, at]
        if name == 'lin':
            return refs[1].at[:, at]
        return refs[2].at[at, pl.ds(0 if name == 'dna' else zh, zh)]

    def remote(src, dst, send, recv, to_rank):
        return pltpu.make_async_remote_copy(src_ref=src, dst_ref=dst, send_sem=send, recv_sem=recv, device_id={'ep': to_rank}, device_id_type=MESH)

    shared = (su, sl, sd)
    hot = (hu, hl, hd)
    own = {'up': wsu, 'lin': wsl, 'dna': wsd.at[:, pl.ds(0, zh)], 'dnb': wsd.at[:, pl.ds(zh, zh)]}

    full = (wu.at[0], wl.at[0], wd.at[0])

    def half_of(n, c):
        return full[n].at[:, pl.ds(c * half, half)] if n < 2 else full[n].at[pl.ds(c * half, half), :]

    far = [remote(half_of(n, 1), hot[n], far_send.at[n], far_recv.at[n], 1) for n in range(3)]

    @pl.when(rank == 0)
    def _():
        for copy in far:
            copy.start()

    first, second, third = [], [], []
    for n, (name, axis) in enumerate(PIECES):
        near, other = (x_chip, y_chip) if axis == 'x' else (y_chip, x_chip)
        here = region(shared, name, chip)
        first.append(remote(own[name], here, ag_send.at[n], ag_recv.at[n], near * 2 + core))
        second.append(remote(own[name], here, ag_send.at[4 + n], ag_recv.at[4 + n], other * 2 + core))
        got = region(shared, name, near)
        third.append(remote(got, got, ag_send.at[8 + n], ag_recv.at[8 + n], other * 2 + core))
    for copy in first + second:
        copy.start()
    local = [(wsu, small_a.at[0], region(shared, 'up', chip)), (wsl, small_a.at[1], region(shared, 'lin', chip)), (wsd, small_b, sd.at[pl.ds(pl.multiple_of(chip * part, 128), part), :])]
    loads = [pltpu.make_async_copy(src, mid, load_sem.at[n]) for n, (src, mid, _) in enumerate(local)]
    stores = [pltpu.make_async_copy(mid, dst, store_sem.at[n]) for n, (_, mid, dst) in enumerate(local)]
    mids = (big_a.at[0], big_a.at[1], big_b)
    own_loads = [pltpu.make_async_copy(half_of(n, 0), mids[n], load_sem.at[3 + n]) for n in range(3)]
    own_stores = [pltpu.make_async_copy(mids[n], hot[n], store_sem.at[3 + n]) for n in range(3)]
    for copy in loads:
        copy.start()

    @pl.when(rank == 0)
    def _():
        for copy in own_loads:
            copy.start()

    chunks = [(name, axis, slot) for slot in range(4) for name, axis in PIECES]

    def hot_copy(n, to_chip, source):
        name, axis, slot = chunks[n]
        return remote(region(source, name, slot), region(hot, name, slot), hot_send.at[n], hot_recv.at[n], to_chip * 2 + core)

    route = {'x': {0: 1, 1: 3, 3: 2}, 'y': {0: 2, 2: 3, 3: 1}}

    @pl.when(rank == 0)
    def _():
        lo = (full[0].at[:, pl.ds(0, half)], full[1].at[:, pl.ds(0, half)], full[2].at[pl.ds(0, half), :])
        for n, (name, axis, slot) in enumerate(chunks):
            hot_copy(n, route[axis][0], lo).start()

    @pl.when(rank == 1)
    def _():
        for n in range(3):
            far[n].wait_recv()
        for n, (name, axis, slot) in enumerate(chunks):
            hot_copy(n, route[axis][0], hot).start()

    for n, copy in enumerate(first):
        copy.wait_recv()
        third[n].start()
    for n in range(3):
        loads[n].wait()
        stores[n].start()

    @pl.when(rank == 0)
    def _():
        for n in range(3):
            own_loads[n].wait()
            own_stores[n].start()

    for me in (1, 2, 3):
        @pl.when(chip == me)
        def _():
            for n, (name, axis, slot) in enumerate(chunks):
                if me in route[axis]:
                    hot_copy(n, 0, hot).wait_recv()
                    hot_copy(n, route[axis][me], hot).start()
            for n, (name, axis, slot) in enumerate(chunks):
                if me not in route[axis]:
                    hot_copy(n, 0, hot).wait_recv()

    for me in (0, 1, 2, 3):
        @pl.when(chip == me)
        def _():
            for n, (name, axis, slot) in enumerate(chunks):
                if me in route[axis]:
                    hot_copy(n, route[axis][me], hot).wait_send()

    for copy in first:
        copy.wait_send()
    for copy in second + third:
        copy.wait()
    for copy in stores:
        copy.wait()

    @pl.when(rank == 0)
    def _():
        for n in range(3):
            far[n].wait_send()
            own_stores[n].wait()


def weights_call(ws_up, ws_lin, ws_down, w_up, w_lin, w_down):
    width, part = ws_up.shape
    half = 4 * part
    hbm = pl.BlockSpec(memory_space=pl.ANY)
    shapes = [jax.ShapeDtypeStruct(v, BF16) for v in ((width, half), (width, half), (half, width))]
    dma = pltpu.SemaphoreType.DMA
    return pl.pallas_call(
        functools.partial(weights_kernel, part),
        in_specs=[hbm] * 6,
        out_specs=[hbm] * 6,
        out_shape=shapes + shapes,
        scratch_shapes=[
            pltpu.VMEM((2, width, part), BF16), pltpu.VMEM((part, width), BF16), pltpu.VMEM((2, width, half), BF16), pltpu.VMEM((half, width), BF16),
            dma((6,)), dma((6,)), dma((3,)), dma((3,)), dma((12,)), dma((12,)), dma((16,)), dma((16,)),
        ],
        cost_estimate=pl.CostEstimate(flops=10 ** 11, bytes_accessed=5 * 10 ** 7, transcendentals=0),
        compiler_params=pltpu.CompilerParams(has_side_effects=True, vmem_limit_bytes=48 * 1024 * 1024),
    )(ws_up, ws_lin, ws_down, w_up, w_lin, w_down)


def place_kernel(plans, count, *refs):
    owner = lax.axis_index('ep') == 0
    zc = lax.axis_index('dp')
    sources, outs = refs[:count], refs[count + 3:count + 6]
    hold, in_sem, out_sem = refs[count + 6:]
    side = hold.shape[1]

    def pull(n):
        which, src, row, _, _, _ = plans[n]
        return pltpu.make_async_copy(sources[src].at[pl.ds(row, side)], hold.at[n], in_sem.at[n])

    def push(n):
        which, _, _, z_rel, slot, slot_dim = plans[n]
        zpos = (zc if z_rel == 0 else 1 - zc) * side
        where = (pl.ds(zpos, side), pl.ds(slot, side)) if slot_dim == 1 else (pl.ds(slot, side), pl.ds(pl.multiple_of(zpos, 128), side))
        return pltpu.make_async_copy(hold.at[n], outs[which].at[(0,) + where], out_sem.at[n])

    @pl.when(owner)
    def _():
        for n in range(len(plans)):
            pull(n).start()
        for n in range(len(plans)):
            pull(n).wait()
            push(n).start()
        for n in range(len(plans)):
            push(n).wait()


def place_call(states, norms, slot_dims, part):
    sources, plans, known = [], [], {}
    for which, (state, slot_dim) in enumerate(zip(states, slot_dims)):
        for (c, y, x, z), (array, row) in sorted(state.items()):
            if id(array) not in known:
                known[id(array)] = len(sources)
                sources.append(array)
            plans.append((which, known[id(array)], row, z, (c * 4 + y * 2 + x) * part, slot_dim))
    side = sources[0].shape[1]
    hbm = pl.BlockSpec(memory_space=pl.ANY)
    return pl.pallas_call(
        functools.partial(place_kernel, tuple(plans), len(sources)),
        in_specs=[hbm] * (len(sources) + 3),
        out_specs=[hbm] * 3,
        out_shape=[jax.ShapeDtypeStruct(v.shape, v.dtype) for v in norms],
        scratch_shapes=[pltpu.VMEM((len(plans), side, side), F32), pltpu.SemaphoreType.DMA((len(plans),)), pltpu.SemaphoreType.DMA((len(plans),))],
        input_output_aliases={len(sources) + k: k for k in range(3)},
        cost_estimate=pl.CostEstimate(flops=2 * 10 ** 10, bytes_accessed=57 * 10 ** 6, transcendentals=0),
        compiler_params=pltpu.CompilerParams(vmem_limit_bytes=48 * 1024 * 1024),
    )(*sources, *norms)


def solution(mesh):
    dp_size, ep_size = mesh.shape['dp'], mesh.shape['ep']
    total = dp_size * ep_size
    both = ('dp', 'ep')

    def swap(value, axis):
        bit = ep_size if axis == 'z' else BIT[axis]
        return lax.ppermute(value, both, [(i, i ^ bit) for i in range(total)])

    def move(value, pairs):
        return lax.ppermute(value, both, [(z * ep_size + s, z * ep_size + d) for z in range(dp_size) for s, d in pairs])

    def local_step(hidden, route_idx, gates, grad_out, w_up, w_lin, w_down, ws_up, ws_lin, ws_down):
        tok, width = hidden.shape
        ff = w_up.shape[2]
        part = ff // ep_size
        half = ff // 2
        zh = width // 2
        cap = (tok + ep_size - 2) // (ep_size - 1)
        cap = (cap + 7) // 8 * 8
        rank = lax.axis_index('ep')
        zc = lax.axis_index('dp')
        core0 = rank % 2 == 0
        x0 = (rank // 2) % 2 == 0
        y0 = rank // 4 == 0
        is_owner = rank == 0

        s_up, s_lin, s_dn, h_up, h_lin, h_dn = weights_call(ws_up, ws_lin, ws_down, w_up, w_lin, w_down)
        route_idx, gates, hidden, grad_out = lax.optimization_barrier((route_idx, gates, hidden, grad_out, s_up))[:4]

        ids = route_idx.reshape(-1)
        is_hot = ids == HOT
        gate = gates.astype(F32)
        d_tok = (gate * grad_out.astype(F32)).astype(BF16)
        d_hot = jnp.where(is_hot[:, None], d_tok, jnp.zeros_like(d_tok))
        onehot = (ids[:, None] == jnp.arange(ep_size)[None, :]).astype(jnp.int32)
        before = jnp.cumsum(onehot, axis=0) - onehot
        pos_in = jnp.sum(before * onehot, axis=1)
        slots = ep_size * cap
        dest = jnp.where(is_hot, slots, ids * cap + pos_in)
        src_map = jnp.zeros((slots,), jnp.int32).at[dest].set(jnp.arange(tok, dtype=jnp.int32) + 1, mode='drop')

        pair = lambda rows: jnp.concatenate([rows, swap(rows, 'c')], axis=0)
        x2, dy2, dh2 = pair(hidden), pair(grad_out), pair(d_hot)

        def after(values, token):
            return lax.optimization_barrier((values, token))[0]

        def join(partial):
            return partial[:tok] + swap(partial[tok:], 'c')

        def local_rows(d_rows, up_w, lin_w, dn_w):
            return expert_call(x2, d_rows, up_w, lin_w, dn_w, F32, 512, 2 * tok)

        def local_grads(rows, d_rows, saved):
            act, d_up, d_lin = saved[:3]
            return [mm(rows, d_up, 0, 0), mm(rows, d_lin, 0, 0), mm(act, d_rows, 0, 0)]

        SLOT_DIMS = (1, 1, 0)
        ORDERS = ('xyz', 'yzx', 'zxy')

        def split(grad, slot_dim, axis, slots_here):
            cut = lambda v, k: lax.slice_in_dim(v, k * part, (k + 1) * part, axis=slot_dim)
            if axis == 'z':
                take = lambda k: lax.dynamic_slice_in_dim(grad, k * zh, zh, axis=1 - slot_dim)
                return take(1 - zc), take(zc), slots_here
            bit = 1 if axis == 'x' else 2
            low = [k for k, q in enumerate(slots_here) if not q & bit]
            high = [k for k, q in enumerate(slots_here) if q & bit]
            low_cut = jnp.concatenate([cut(grad, k) for k in low], axis=slot_dim)
            high_cut = jnp.concatenate([cut(grad, k) for k in high], axis=slot_dim)
            lower = x0 if axis == 'x' else y0
            return jnp.where(lower, high_cut, low_cut), jnp.where(lower, low_cut, high_cut), [slots_here[k] for k in low]

        class Reduction:
            def __init__(self, grads):
                self.now, self.slots, self.step = list(grads), [[0, 1, 2, 3]] * 3, 0

            def start(self):
                self.keep, self.got = [None] * 3, [None] * 3
                for n in range(3):
                    axis = ORDERS[n][self.step]
                    send, self.keep[n], self.slots[n] = split(self.now[n], SLOT_DIMS[n], axis, self.slots[n])
                    self.got[n] = swap(send, axis)
                self.step += 1

            def finish(self, token):
                self.got = after(self.got, token)
                self.now = [keep + got for keep, got in zip(self.keep, self.got)]

        EVEN = [0, 2, 4, 6]

        class ToOwner:
            def __init__(self, blocks):
                self.state, self.live, self.step = [], [EVEN] * 3, 0
                for block in blocks:
                    self.state.append({(0, 0, 0, 0): (block, 0), (1, 0, 0, 0): (move(block, [(r + 1, r) for r in EVEN]), 0)})

            def start(self):
                self.got = [None] * 3
                for n in range(3):
                    axis, state, live = ('zyx', 'xzy', 'yxz')[n][self.step], self.state[n], self.live[n]
                    packed = jnp.concatenate([state[k][0][state[k][1]:state[k][1] + zh] for k in sorted(state)], axis=0)
                    if axis == 'z':
                        self.got[n] = lax.ppermute(packed, both, [(z * ep_size + r, (1 - z) * ep_size + r) for z in range(dp_size) for r in live])
                    else:
                        self.got[n] = move(packed, [(r, r - BIT[axis]) for r in live if r & BIT[axis]])
                        self.live[n] = [r for r in live if not r & BIT[axis]]

            def finish(self, token):
                self.got = after(self.got, token)
                for n in range(3):
                    dim = {'y': 1, 'x': 2, 'z': 3}[('zyx', 'xzy', 'yxz')[n][self.step]]
                    for m, k in enumerate(sorted(self.state[n])):
                        self.state[n][k[:dim] + (1,) + k[dim + 1:]] = (self.got[n], m * zh)
                self.step += 1

        rows = jnp.take(jnp.concatenate([hidden, d_tok], axis=1), jnp.maximum(src_map - 1, 0), axis=0)
        rows = rows * (src_map > 0).astype(BF16)[:, None]
        mine = lax.all_to_all(rows.reshape(ep_size, cap, 2 * width), 'ep', 0, 0, tiled=True).reshape(slots, 2 * width)
        far = swap(mine, 'z')
        tile = slots // 2

        h_rows = local_rows(dh2, h_up, h_lin, h_dn)
        h_grads = local_grads(x2, dh2, h_rows)
        h_sum = Reduction(h_grads)
        h_sum.start()

        dy2 = after(dy2, h_grads)
        s_rows = local_rows(dy2, s_up, s_lin, s_dn)
        h_sum.finish(s_rows[0])
        h_sum.start()

        s_x2, s_act = after((x2, s_rows[0]), h_sum.keep)
        s_grads = local_grads(s_x2, dy2, [s_act] + list(s_rows[1:3]))
        h_sum.finish(s_grads)
        h_sum.start()

        mine = after(mine, h_sum.keep)
        *saved, n_out, n_dx = expert_call(mine[:, :width], mine[:, width:], w_up[0], w_lin[0], w_down[0], BF16, tile, 2 * slots)
        h_sum.finish(s_grads)
        owner = ToOwner(h_sum.now)
        owner.start()
        owner.finish(saved[0])
        back = jnp.concatenate([n_out, n_dx], axis=1).reshape(ep_size, cap, 2 * width)
        back = lax.all_to_all(back, 'ep', 0, 0, tiled=True).reshape(slots, 2 * width)
        owner.start()

        far = after(far, saved[0])
        saved = expert_call(far[:, :width], far[:, width:], w_up[0], w_lin[0], w_down[0], BF16, tile, 2 * slots, tuple(saved))
        owner.finish(saved[0])
        owner.start()

        n_x = jnp.concatenate([mine[:, :width], far[:, :width]], axis=0)
        n_d = jnp.concatenate([mine[:, width:], far[:, width:]], axis=0)
        n_grads = local_grads(n_x, n_d, saved)
        s_grads = after(s_grads, saved[0])
        s_sum = Reduction(s_grads)
        s_sum.start()
        owner.finish(n_grads)
        dw = place_call(owner.state, [g[None] for g in n_grads], SLOT_DIMS, part)

        h_out, h_dx = join(h_rows[3]), join(h_rows[4])
        s_out, s_dx = join(s_rows[3]), join(s_rows[4])
        s_sum.finish(n_grads)
        s_sum.start()
        back = jnp.take(back, jnp.minimum(dest, slots - 1), axis=0)
        s_sum.finish(n_grads)
        s_sum.start()
        s_sum.finish(dw)

        def z_join(block, dim):
            got = swap(block, 'z')
            return jnp.where(zc == 0, jnp.concatenate([block, got], axis=dim), jnp.concatenate([got, block], axis=dim))

        dws = [z_join(s_sum.now[0], 0), z_join(s_sum.now[1], 0), z_join(s_sum.now[2], 1)]

        hot_row = is_hot[:, None]
        rounded = lambda v: lax.reduce_precision(v, exponent_bits=8, mantissa_bits=7)
        o_tok = jnp.where(hot_row, rounded(h_out), back[:, :width].astype(F32))
        p_tok = jnp.where(hot_row, rounded(h_dx), back[:, width:].astype(F32))
        y_tok = (gate * o_tok + s_out).astype(BF16)
        d_hidden = (p_tok + s_dx).astype(BF16)
        return (y_tok, d_hidden, dw[0], dw[1], dw[2], dws[0], dws[1], dws[2])

    tok_spec = P(both, None)
    expert_spec = P('ep', None, None)
    col_spec = P(None, 'ep')
    row_spec = P('ep', None)
    return jax.shard_map(local_step, mesh=mesh, in_specs=(tok_spec, tok_spec, tok_spec, tok_spec, expert_spec, expert_spec, expert_spec, col_spec, col_spec, row_spec), out_specs=(tok_spec, tok_spec, expert_spec, expert_spec, expert_spec, col_spec, col_spec, row_spec), check_vma=False)
```

```python
import functools

import jax
import jax.numpy as jnp
from jax import lax
from jax.experimental import pallas as pl
from jax.experimental.pallas import tpu as pltpu
from jax.sharding import PartitionSpec as P


HOT = 0
F32 = jnp.float32
BF16 = jnp.bfloat16
BIT = {'c': 1, 'x': 2, 'y': 4}


def mm(a, b, ca, cb):
    return lax.dot_general(a, b, (((ca,), (cb,)), ((), ())), preferred_element_type=F32)


def expert_tile(first, halves, x_ref, d_ref, up_ref, lin_ref, dn_ref, *rest):
    row, col = pl.program_id(0), pl.program_id(1)
    if first:
        act_ref, du_ref, dl_ref = rest[:3]
        outs, dxs = rest[3:3 + halves], rest[3 + halves:3 + 2 * halves]
        out_acc, dx_acc = rest[3 + 2 * halves:]
    else:
        act_ref, du_ref, dl_ref = rest[-3:]
    up = mm(x_ref[...], up_ref[...], 1, 0)
    lin = mm(x_ref[...], lin_ref[...], 1, 0)
    d_act = mm(d_ref[...], dn_ref[...], 1, 1)
    sig = jax.nn.sigmoid(up)
    silu = up * sig
    act = (silu * lin).astype(BF16)
    d_up = (d_act * lin * sig * (1.0 + up * (1.0 - sig))).astype(BF16)
    d_lin = (d_act * silu).astype(BF16)
    act_ref[...] = act
    du_ref[...] = d_up
    dl_ref[...] = d_lin
    if first:
        out_part = mm(act, dn_ref[...], 1, 0)
        dx_part = mm(d_up, up_ref[...], 1, 1) + mm(d_lin, lin_ref[...], 1, 1)

        @pl.when(col == 0)
        def _():
            out_acc[...] = out_part
            dx_acc[...] = dx_part

        @pl.when(col > 0)
        def _():
            out_acc[...] += out_part
            dx_acc[...] += dx_part

        for part in range(halves):
            share = pl.num_programs(0) // halves

            @pl.when((col == pl.num_programs(1) - 1) & (row >= part * share) & (row < (part + 1) * share))
            def _():
                outs[part][...] = out_acc[...].astype(outs[part].dtype)
                dxs[part][...] = dx_acc[...].astype(dxs[part].dtype)


def expert_call(x, d, cols, up_w, lin_w, dn_w, out_type, tile, total_rows, halves=1, saved=None):
    rows, width = x.shape[0], up_w.shape[0]
    ff = up_w.shape[1]
    ft = 512
    first = saved is None
    offset = 0 if first else rows // tile
    count = rows // tile
    wide = pl.BlockSpec((tile, ft), lambda r, c: (r + offset, c))
    in_specs = [pl.BlockSpec((tile, width), lambda r, c: (r, cols[0])), pl.BlockSpec((tile, width), lambda r, c: (r, cols[1]))]
    in_specs += [pl.BlockSpec((width, ft), lambda r, c: (0, c)), pl.BlockSpec((width, ft), lambda r, c: (0, c)), pl.BlockSpec((ft, width), lambda r, c: (c, 0))]
    out_shape = [jax.ShapeDtypeStruct((total_rows, ff), BF16)] * 3
    out_specs = [wide] * 3
    scratch, alias, extra = [], {}, ()
    if first:
        share = count // halves
        thin = [pl.BlockSpec((tile, width), lambda r, c, p=p: (jnp.clip(r - p * share, 0, share - 1), 0)) for p in range(halves)]
        out_shape += [jax.ShapeDtypeStruct((rows // halves, width), out_type)] * (2 * halves)
        out_specs += thin * 2
        scratch = [pltpu.VMEM((tile, width), F32)] * 2
    else:
        extra = saved
        in_specs += [pl.BlockSpec(memory_space=pl.ANY)] * 3
        alias = {5: 0, 6: 1, 7: 2}
    flops = 2 * rows * width * ff * (6 if first else 3)
    return pl.pallas_call(
        functools.partial(expert_tile, first, halves),
        grid=(count, ff // ft),
        in_specs=in_specs,
        out_specs=out_specs,
        out_shape=out_shape,
        scratch_shapes=scratch,
        input_output_aliases=alias,
        cost_estimate=pl.CostEstimate(flops=flops, bytes_accessed=6 * rows * ff, transcendentals=rows * ff),
        compiler_params=pltpu.CompilerParams(dimension_semantics=('arbitrary', 'arbitrary'), vmem_limit_bytes=60 * 1024 * 1024),
    )(x, d, up_w, lin_w, dn_w, *extra)


MESH = pl.DeviceIdType.MESH
PIECES = (('up', 'x'), ('lin', 'y'), ('dna', 'x'), ('dnb', 'y'))
SHARED = (('up', 'x', 0), ('lin', 'x', 1), ('dna', 'y', 0), ('dnb', 'y', 1))


def weights_kernel(part, wsu, wsl, wsd, wu, wl, wd, su, sl, sd, hu, hl, hd, small_a, small_b, big_a, big_b, load_sem, store_sem, far_send, far_recv, ag_send, ag_recv, z_send, z_recv, hot_send, hot_recv):
    rank, row = lax.axis_index('ep'), lax.axis_index('dp')
    chip, core = rank // 2, rank % 2
    half, zh = 4 * part, wsd.shape[1] // 2
    xbit, ybit = chip % 2, chip // 2
    x_chip = chip + 1 - 2 * xbit
    y_chip = chip + 2 - 4 * ybit
    xy_chip = 3 - chip

    def region(refs, name, slot):
        at = pl.ds(pl.multiple_of(slot * part, 128), part)
        if name == 'up':
            return refs[0].at[:, at]
        if name == 'lin':
            return refs[1].at[:, at]
        return refs[2].at[at, pl.ds(0 if name == 'dna' else zh, zh)]

    def remote(src, dst, send, recv, to_rank):
        return pltpu.make_async_remote_copy(src_ref=src, dst_ref=dst, send_sem=send, recv_sem=recv, device_id={'ep': to_rank}, device_id_type=MESH)

    shared = (su, sl, sd)
    hot = (hu, hl, hd)
    own = {'up': wsu, 'lin': wsl, 'dna': wsd.at[:, pl.ds(0, zh)], 'dnb': wsd.at[:, pl.ds(zh, zh)]}

    full = (wu.at[0], wl.at[0], wd.at[0])

    def half_of(n, c):
        return full[n].at[:, pl.ds(c * half, half)] if n < 2 else full[n].at[pl.ds(c * half, half), :]

    far = [remote(half_of(n, 1), hot[n], far_send.at[n], far_recv.at[n], 1) for n in range(3)]

    @pl.when(rank == 0)
    def _():
        for copy in far:
            copy.start()

    def ag_copy(n, step):
        name, axis, _ = SHARED[n]
        near, other = (x_chip, y_chip) if axis == 'x' else (y_chip, x_chip)
        src = region(shared, name, near) if step == 2 else own[name]
        dst = region(shared, name, near if step == 2 else chip)
        at = 4 * step + n
        return remote(src, dst, ag_send.at[at], ag_recv.at[at], (other if step else near) * 2 + core)

    def z_copy(n, step):
        name, axis, _ = SHARED[n]
        near, other = (x_chip, y_chip) if axis == 'x' else (y_chip, x_chip)
        at = region(shared, name, (near, other, xy_chip)[step])
        sem = 3 * n + step
        return pltpu.make_async_remote_copy(src_ref=at, dst_ref=at, send_sem=z_send.at[sem], recv_sem=z_recv.at[sem], device_id={'dp': 1 - row}, device_id_type=MESH)

    def in_row(n):
        return row == SHARED[n][2]

    for n in range(4):
        @pl.when(in_row(n))
        def _():
            ag_copy(n, 0).start()
            ag_copy(n, 1).start()
    local = [(wsu, small_a.at[0], region(shared, 'up', chip)), (wsl, small_a.at[1], region(shared, 'lin', chip)), (wsd, small_b, sd.at[pl.ds(pl.multiple_of(chip * part, 128), part), :])]
    loads = [pltpu.make_async_copy(src, mid, load_sem.at[n]) for n, (src, mid, _) in enumerate(local)]
    stores = [pltpu.make_async_copy(mid, dst, store_sem.at[n]) for n, (_, mid, dst) in enumerate(local)]
    mids = (big_a.at[0], big_a.at[1], big_b)
    own_loads = [pltpu.make_async_copy(half_of(n, 0), mids[n], load_sem.at[3 + n]) for n in range(3)]
    own_stores = [pltpu.make_async_copy(mids[n], hot[n], store_sem.at[3 + n]) for n in range(3)]
    for copy in loads:
        copy.start()

    @pl.when(rank == 0)
    def _():
        for copy in own_loads:
            copy.start()

    chunks = [(name, axis, slot) for slot in range(4) for name, axis in PIECES]

    def hot_copy(n, to_chip, source):
        name, axis, slot = chunks[n]
        return remote(region(source, name, slot), region(hot, name, slot), hot_send.at[n], hot_recv.at[n], to_chip * 2 + core)

    route = {'x': {0: 1, 1: 3, 3: 2}, 'y': {0: 2, 2: 3, 3: 1}}

    for n in range(4):
        @pl.when(in_row(n))
        def _():
            ag_copy(n, 0).wait_recv()
            ag_copy(n, 2).start()
            z_copy(n, 0).start()

    @pl.when(rank == 0)
    def _():
        lo = (full[0].at[:, pl.ds(0, half)], full[1].at[:, pl.ds(0, half)], full[2].at[pl.ds(0, half), :])
        for n, (name, axis, slot) in enumerate(chunks):
            hot_copy(n, route[axis][0], lo).start()

    @pl.when(rank == 1)
    def _():
        for n in range(3):
            far[n].wait_recv()
        for n, (name, axis, slot) in enumerate(chunks):
            hot_copy(n, route[axis][0], hot).start()

    for step in (1, 2):
        for n in range(4):
            @pl.when(in_row(n))
            def _():
                ag_copy(n, step).wait_recv()
                z_copy(n, step).start()
    for n in range(3):
        loads[n].wait()
        stores[n].start()

    @pl.when(rank == 0)
    def _():
        for n in range(3):
            own_loads[n].wait()
            own_stores[n].start()

    for me in (1, 2, 3):
        @pl.when(chip == me)
        def _():
            for n, (name, axis, slot) in enumerate(chunks):
                if me in route[axis]:
                    hot_copy(n, 0, hot).wait_recv()
                    hot_copy(n, route[axis][me], hot).start()
            for n, (name, axis, slot) in enumerate(chunks):
                if me not in route[axis]:
                    hot_copy(n, 0, hot).wait_recv()

    for me in (0, 1, 2, 3):
        @pl.when(chip == me)
        def _():
            for n, (name, axis, slot) in enumerate(chunks):
                if me in route[axis]:
                    hot_copy(n, route[axis][me], hot).wait_send()

    for n in range(4):
        @pl.when(in_row(n))
        def _():
            for step in range(3):
                ag_copy(n, step).wait_send()
                z_copy(n, step).wait_send()

        @pl.when(jnp.logical_not(in_row(n)))
        def _():
            for step in range(3):
                z_copy(n, step).wait_recv()
    for copy in stores:
        copy.wait()

    @pl.when(rank == 0)
    def _():
        for n in range(3):
            far[n].wait_send()
            own_stores[n].wait()


def weights_call(ws_up, ws_lin, ws_down, w_up, w_lin, w_down):
    width, part = ws_up.shape
    half = 4 * part
    hbm = pl.BlockSpec(memory_space=pl.ANY)
    shapes = [jax.ShapeDtypeStruct(v, BF16) for v in ((width, half), (width, half), (half, width))]
    dma = pltpu.SemaphoreType.DMA
    return pl.pallas_call(
        functools.partial(weights_kernel, part),
        in_specs=[hbm] * 6,
        out_specs=[hbm] * 6,
        out_shape=shapes + shapes,
        scratch_shapes=[
            pltpu.VMEM((2, width, part), BF16), pltpu.VMEM((part, width), BF16), pltpu.VMEM((2, width, half), BF16), pltpu.VMEM((half, width), BF16),
            dma((6,)), dma((6,)), dma((3,)), dma((3,)), dma((12,)), dma((12,)), dma((12,)), dma((12,)), dma((16,)), dma((16,)),
        ],
        cost_estimate=pl.CostEstimate(flops=10 ** 11, bytes_accessed=5 * 10 ** 7, transcendentals=0),
        compiler_params=pltpu.CompilerParams(has_side_effects=True, vmem_limit_bytes=48 * 1024 * 1024),
    )(ws_up, ws_lin, ws_down, w_up, w_lin, w_down)


def place_kernel(plans, count, *refs):
    owner = lax.axis_index('ep') == 0
    zc = lax.axis_index('dp')
    sources, outs = refs[:count], refs[count + 3:count + 6]
    hold, in_sem, out_sem = refs[count + 6:]
    side = hold.shape[1]

    def pull(n):
        which, src, row, _, _, _ = plans[n]
        return pltpu.make_async_copy(sources[src].at[pl.ds(row, side)], hold.at[n], in_sem.at[n])

    def push(n):
        which, _, _, z_rel, slot, slot_dim = plans[n]
        zpos = (zc if z_rel == 0 else 1 - zc) * side
        where = (pl.ds(zpos, side), pl.ds(slot, side)) if slot_dim == 1 else (pl.ds(slot, side), pl.ds(pl.multiple_of(zpos, 128), side))
        return pltpu.make_async_copy(hold.at[n], outs[which].at[(0,) + where], out_sem.at[n])

    @pl.when(owner)
    def _():
        for n in range(len(plans)):
            pull(n).start()
        for n in range(len(plans)):
            pull(n).wait()
            push(n).start()
        for n in range(len(plans)):
            push(n).wait()


def place_call(states, norms, slot_dims, part):
    sources, plans, known = [], [], {}
    for which, (state, slot_dim) in enumerate(zip(states, slot_dims)):
        for (c, y, x, z), (array, row) in sorted(state.items()):
            if id(array) not in known:
                known[id(array)] = len(sources)
                sources.append(array)
            plans.append((which, known[id(array)], row, z, (c * 4 + y * 2 + x) * part, slot_dim))
    side = sources[0].shape[1]
    hbm = pl.BlockSpec(memory_space=pl.ANY)
    return pl.pallas_call(
        functools.partial(place_kernel, tuple(plans), len(sources)),
        in_specs=[hbm] * (len(sources) + 3),
        out_specs=[hbm] * 3,
        out_shape=[jax.ShapeDtypeStruct(v.shape, v.dtype) for v in norms],
        scratch_shapes=[pltpu.VMEM((len(plans), side, side), F32), pltpu.SemaphoreType.DMA((len(plans),)), pltpu.SemaphoreType.DMA((len(plans),))],
        input_output_aliases={len(sources) + k: k for k in range(3)},
        cost_estimate=pl.CostEstimate(flops=2 * 10 ** 10, bytes_accessed=57 * 10 ** 6, transcendentals=0),
        compiler_params=pltpu.CompilerParams(vmem_limit_bytes=48 * 1024 * 1024),
    )(*sources, *norms)


def solution(mesh):
    dp_size, ep_size = mesh.shape['dp'], mesh.shape['ep']
    total = dp_size * ep_size
    both = ('dp', 'ep')

    def swap(value, axis):
        bit = ep_size if axis == 'z' else BIT[axis]
        return lax.ppermute(value, both, [(i, i ^ bit) for i in range(total)])

    def move(value, pairs):
        return lax.ppermute(value, both, [(z * ep_size + s, z * ep_size + d) for z in range(dp_size) for s, d in pairs])

    def local_step(hidden, route_idx, gates, grad_out, w_up, w_lin, w_down, ws_up, ws_lin, ws_down):
        tok, width = hidden.shape
        ff = w_up.shape[2]
        part = ff // ep_size
        half = ff // 2
        zh = width // 2
        cap = (tok + ep_size - 2) // (ep_size - 1)
        cap = (cap + 7) // 8 * 8
        rank = lax.axis_index('ep')
        zc = lax.axis_index('dp')
        core0 = rank % 2 == 0
        x0 = (rank // 2) % 2 == 0
        y0 = rank // 4 == 0
        is_owner = rank == 0

        s_up, s_lin, s_dn, h_up, h_lin, h_dn = weights_call(ws_up, ws_lin, ws_down, w_up, w_lin, w_down)
        route_idx, gates, hidden, grad_out = lax.optimization_barrier((route_idx, gates, hidden, grad_out, s_up))[:4]

        ids = route_idx.reshape(-1)
        is_hot = ids == HOT
        gate = gates.astype(F32)
        d_tok = (gate * grad_out.astype(F32)).astype(BF16)
        d_hot = jnp.where(is_hot[:, None], d_tok, jnp.zeros_like(d_tok))
        onehot = (ids[:, None] == jnp.arange(ep_size)[None, :]).astype(jnp.int32)
        before = jnp.cumsum(onehot, axis=0) - onehot
        pos_in = jnp.sum(before * onehot, axis=1)
        slots = ep_size * cap
        dest = jnp.where(is_hot, slots, ids * cap + pos_in)
        src_map = jnp.zeros((slots,), jnp.int32).at[dest].set(jnp.arange(tok, dtype=jnp.int32) + 1, mode='drop')

        pair = lambda rows: jnp.concatenate([rows, swap(rows, 'c')], axis=0)
        x2, dy2, dh2 = pair(hidden), pair(grad_out), pair(d_hot)

        def after(values, token):
            return lax.optimization_barrier((values, token))[0]

        def join(own, partner):
            return own + swap(partner, 'c')

        def local_rows(d_rows, up_w, lin_w, dn_w):
            return expert_call(x2, d_rows, (0, 0), up_w, lin_w, dn_w, F32, 512, 2 * tok, 2)

        def local_grads(rows, d_rows, saved):
            act, d_up, d_lin = saved[:3]
            return [mm(rows, d_up, 0, 0), mm(rows, d_lin, 0, 0), mm(act, d_rows, 0, 0)]

        SLOT_DIMS = (1, 1, 0)
        ORDERS = ('xyz', 'yzx', 'zxy')

        def split(grad, slot_dim, axis, slots_here):
            cut = lambda v, k: lax.slice_in_dim(v, k * part, (k + 1) * part, axis=slot_dim)
            if axis == 'z':
                take = lambda k: lax.dynamic_slice_in_dim(grad, k * zh, zh, axis=1 - slot_dim)
                return take(1 - zc), take(zc), slots_here
            bit = 1 if axis == 'x' else 2
            low = [k for k, q in enumerate(slots_here) if not q & bit]
            high = [k for k, q in enumerate(slots_here) if q & bit]
            low_cut = jnp.concatenate([cut(grad, k) for k in low], axis=slot_dim)
            high_cut = jnp.concatenate([cut(grad, k) for k in high], axis=slot_dim)
            lower = x0 if axis == 'x' else y0
            return jnp.where(lower, high_cut, low_cut), jnp.where(lower, low_cut, high_cut), [slots_here[k] for k in low]

        class Reduction:
            def __init__(self, grads):
                self.now, self.slots, self.step = list(grads), [[0, 1, 2, 3]] * 3, 0

            def start(self):
                self.keep, self.got = [None] * 3, [None] * 3
                for n in range(3):
                    axis = ORDERS[n][self.step]
                    send, self.keep[n], self.slots[n] = split(self.now[n], SLOT_DIMS[n], axis, self.slots[n])
                    self.got[n] = swap(send, axis)
                self.step += 1

            def finish(self, token):
                self.got = after(self.got, token)
                self.now = [keep + got for keep, got in zip(self.keep, self.got)]

        EVEN = [0, 2, 4, 6]

        class ToOwner:
            def __init__(self, blocks):
                self.live, self.step = [EVEN] * 3, 0
                self.have = [[block, move(block, [(r + 1, r) for r in EVEN])] for block in blocks]
                self.keys = [[(0, 0, 0, 0), (1, 0, 0, 0)] for _ in blocks]

            def start(self):
                for n in range(3):
                    axis, live = ('zyx', 'xzy', 'yxz')[n][self.step], self.live[n]
                    packed = jnp.concatenate(self.have[n], axis=0)
                    if axis == 'z':
                        got = lax.ppermute(packed, both, [(z * ep_size + r, (1 - z) * ep_size + r) for z in range(dp_size) for r in live])
                    else:
                        got = move(packed, [(r, r - BIT[axis]) for r in live if r & BIT[axis]])
                        self.live[n] = [r for r in live if not r & BIT[axis]]
                    dim = {'y': 1, 'x': 2, 'z': 3}[axis]
                    self.have[n] = [packed, got]
                    self.keys[n] = self.keys[n] + [k[:dim] + (1,) + k[dim + 1:] for k in self.keys[n]]
                self.step += 1

            def finish(self, token):
                got = after([h[1] for h in self.have], token)
                self.have = [[h[0], g] for h, g in zip(self.have, got)]

            def blocks(self):
                out = []
                for have, keys in zip(self.have, self.keys):
                    rows = have[0].shape[0] // zh
                    out.append({k: (have[m // rows], m % rows * zh) for m, k in enumerate(keys)})
                return out

        rows = jnp.take(jnp.concatenate([hidden, d_tok], axis=1), jnp.maximum(src_map - 1, 0), axis=0)
        rows = rows * (src_map > 0).astype(BF16)[:, None]
        mine = lax.all_to_all(rows.reshape(ep_size, cap, 2 * width), 'ep', 0, 0, tiled=True).reshape(slots, 2 * width)
        far = swap(mine, 'z')
        tile = slots // 2

        dh2 = after(dh2, mine)
        h_rows = local_rows(dh2, h_up, h_lin, h_dn)
        h_grads = local_grads(x2, dh2, h_rows)
        h_sum = Reduction(h_grads)
        h_sum.start()

        dy2 = after(dy2, h_grads)
        s_rows = local_rows(dy2, s_up, s_lin, s_dn)
        h_sum.finish(s_rows[0])
        h_sum.start()

        s_x2, s_act = after((x2, s_rows[0]), h_sum.keep)
        s_grads = local_grads(s_x2, dy2, [s_act] + list(s_rows[1:3]))
        h_sum.finish(s_grads)
        h_sum.start()

        def z_join(block, dim):
            got = swap(block, 'z')
            return jnp.where(zc == 0, jnp.concatenate([block, got], axis=dim), jnp.concatenate([got, block], axis=dim))

        s_sum = Reduction(after(s_grads, h_sum.keep))
        s_sum.start()

        mine = after(mine, s_sum.keep)
        *saved, n_out, n_dx = expert_call(mine, mine, (0, 1), w_up[0], w_lin[0], w_down[0], BF16, tile, 2 * slots)
        h_sum.finish(saved[0])
        owner = ToOwner(h_sum.now)
        owner.start()
        s_sum.finish(saved[0])
        s_sum.start()
        back = jnp.concatenate([n_out, n_dx], axis=1).reshape(ep_size, cap, 2 * width)
        back = lax.all_to_all(back, 'ep', 0, 0, tiled=True).reshape(slots, 2 * width)

        far = after(far, (saved[0], s_sum.keep))
        saved = expert_call(far, far, (0, 1), w_up[0], w_lin[0], w_down[0], BF16, tile, 2 * slots, 1, tuple(saved))
        owner.finish(saved[0])
        owner.start()
        s_sum.finish(saved[0])
        s_sum.start()

        n_rows = jnp.concatenate([mine, far], axis=0)
        n_x, n_d = after((n_rows[:, :width], n_rows[:, width:]), s_sum.keep)
        g_up = mm(n_x, saved[1], 0, 0)
        owner.finish(g_up)
        owner.start()
        s_sum.finish(g_up)
        dws = [z_join(s_sum.now[0], 0), z_join(s_sum.now[1], 0), z_join(s_sum.now[2], 1)]
        n_x, n_d = after((n_x, n_d), owner.have[0][0])
        n_grads = [g_up, mm(n_x, saved[2], 0, 0), mm(saved[0], n_d, 0, 0)]
        owner.finish(n_grads)
        dw = place_call(owner.blocks(), [g[None] for g in n_grads], SLOT_DIMS, part)

        h_out, h_dx = join(*h_rows[3:5]), join(*h_rows[5:7])
        s_out, s_dx = join(*s_rows[3:5]), join(*s_rows[5:7])
        back = jnp.take(back, jnp.minimum(dest, slots - 1), axis=0)

        hot_row = is_hot[:, None]
        rounded = lambda v: lax.reduce_precision(v, exponent_bits=8, mantissa_bits=7)
        o_tok = jnp.where(hot_row, rounded(h_out), back[:, :width].astype(F32))
        p_tok = jnp.where(hot_row, rounded(h_dx), back[:, width:].astype(F32))
        y_tok = (gate * o_tok + s_out).astype(BF16)
        d_hidden = (p_tok + s_dx).astype(BF16)
        return (y_tok, d_hidden, dw[0], dw[1], dw[2], dws[0], dws[1], dws[2])

    tok_spec = P(both, None)
    expert_spec = P('ep', None, None)
    col_spec = P(None, 'ep')
    row_spec = P('ep', None)
    return jax.shard_map(local_step, mesh=mesh, in_specs=(tok_spec, tok_spec, tok_spec, tok_spec, expert_spec, expert_spec, expert_spec, col_spec, col_spec, row_spec), out_specs=(tok_spec, tok_spec, expert_spec, expert_spec, expert_spec, col_spec, col_spec, row_spec), check_vma=False)
```

```python
import functools

import jax
import jax.numpy as jnp
from jax import lax
from jax.experimental import pallas as pl
from jax.experimental.pallas import tpu as pltpu
from jax.sharding import PartitionSpec as P


HOT = 0
F32 = jnp.float32
BF16 = jnp.bfloat16
BIT = {'c': 1, 'x': 2, 'y': 4}


def mm(a, b, ca, cb):
    return lax.dot_general(a, b, (((ca,), (cb,)), ((), ())), preferred_element_type=F32)


def expert_tile(first, halves, x_ref, d_ref, up_ref, lin_ref, dn_ref, *rest):
    row, col = pl.program_id(0), pl.program_id(1)
    if first:
        act_ref, du_ref, dl_ref = rest[:3]
        outs, dxs = rest[3:3 + halves], rest[3 + halves:3 + 2 * halves]
        out_acc, dx_acc = rest[3 + 2 * halves:]
    else:
        act_ref, du_ref, dl_ref = rest[-3:]
    up = mm(x_ref[...], up_ref[...], 1, 0)
    lin = mm(x_ref[...], lin_ref[...], 1, 0)
    d_act = mm(d_ref[...], dn_ref[...], 1, 1)
    sig = jax.nn.sigmoid(up)
    silu = up * sig
    act = (silu * lin).astype(BF16)
    d_up = (d_act * lin * sig * (1.0 + up * (1.0 - sig))).astype(BF16)
    d_lin = (d_act * silu).astype(BF16)
    act_ref[...] = act
    du_ref[...] = d_up
    dl_ref[...] = d_lin
    if first:
        out_part = mm(act, dn_ref[...], 1, 0)
        dx_part = mm(d_up, up_ref[...], 1, 1) + mm(d_lin, lin_ref[...], 1, 1)

        @pl.when(col == 0)
        def _():
            out_acc[...] = out_part
            dx_acc[...] = dx_part

        @pl.when(col > 0)
        def _():
            out_acc[...] += out_part
            dx_acc[...] += dx_part

        for part in range(halves):
            share = pl.num_programs(0) // halves

            @pl.when((col == pl.num_programs(1) - 1) & (row >= part * share) & (row < (part + 1) * share))
            def _():
                outs[part][...] = out_acc[...].astype(outs[part].dtype)
                dxs[part][...] = dx_acc[...].astype(dxs[part].dtype)


def expert_call(x, d, cols, up_w, lin_w, dn_w, out_type, tile, total_rows, halves=1, saved=None):
    rows, width = x.shape[0], up_w.shape[0]
    ff = up_w.shape[1]
    ft = ff // 2 if halves == 2 else 512
    first = saved is None
    offset = 0 if first else rows // tile
    count = rows // tile
    wide = pl.BlockSpec((tile, ft), lambda r, c: (r + offset, c))
    in_specs = [pl.BlockSpec((tile, width), lambda r, c: (r, cols[0])), pl.BlockSpec((tile, width), lambda r, c: (r, cols[1]))]
    in_specs += [pl.BlockSpec((width, ft), lambda r, c: (0, c)), pl.BlockSpec((width, ft), lambda r, c: (0, c)), pl.BlockSpec((ft, width), lambda r, c: (c, 0))]
    out_shape = [jax.ShapeDtypeStruct((total_rows, ff), BF16)] * 3
    out_specs = [wide] * 3
    scratch, alias, extra = [], {}, ()
    if first:
        share = count // halves
        thin = [pl.BlockSpec((tile, width), lambda r, c, p=p: (jnp.clip(r - p * share, 0, share - 1), 0)) for p in range(halves)]
        out_shape += [jax.ShapeDtypeStruct((rows // halves, width), out_type)] * (2 * halves)
        out_specs += thin * 2
        scratch = [pltpu.VMEM((tile, width), F32)] * 2
    else:
        extra = saved
        in_specs += [pl.BlockSpec(memory_space=pl.ANY)] * 3
        alias = {5: 0, 6: 1, 7: 2}
    flops = 2 * rows * width * ff * (6 if first else 3)
    return pl.pallas_call(
        functools.partial(expert_tile, first, halves),
        grid=(count, ff // ft),
        in_specs=in_specs,
        out_specs=out_specs,
        out_shape=out_shape,
        scratch_shapes=scratch,
        input_output_aliases=alias,
        cost_estimate=pl.CostEstimate(flops=flops, bytes_accessed=6 * rows * ff, transcendentals=rows * ff),
        compiler_params=pltpu.CompilerParams(dimension_semantics=('arbitrary', 'arbitrary'), vmem_limit_bytes=60 * 1024 * 1024),
    )(x, d, up_w, lin_w, dn_w, *extra)


MESH = pl.DeviceIdType.MESH
PIECES = (('up', 'x'), ('lin', 'y'), ('dna', 'x'), ('dnb', 'y'))
SHARED = (('up', 'x', 0), ('lin', 'x', 1), ('dna', 'y', 0), ('dnb', 'y', 1))


def weights_kernel(part, wsu, wsl, wsd, wu, wl, wd, su, sl, sd, hu, hl, hd, small_a, small_b, big_a, big_b, load_sem, store_sem, far_send, far_recv, ag_send, ag_recv, z_send, z_recv, hot_send, hot_recv):
    rank, row = lax.axis_index('ep'), lax.axis_index('dp')
    chip, core = rank // 2, rank % 2
    half, zh = 4 * part, wsd.shape[1] // 2
    xbit, ybit = chip % 2, chip // 2
    x_chip = chip + 1 - 2 * xbit
    y_chip = chip + 2 - 4 * ybit
    xy_chip = 3 - chip

    def region(refs, name, slot):
        at = pl.ds(pl.multiple_of(slot * part, 128), part)
        if name == 'up':
            return refs[0].at[:, at]
        if name == 'lin':
            return refs[1].at[:, at]
        return refs[2].at[at, pl.ds(0 if name == 'dna' else zh, zh)]

    def strip(refs, name, slot, piece):
        whole = region(refs, name, slot)
        rows = whole.shape[0] // 2
        return whole.at[pl.ds(piece * rows, rows), :]

    def remote(src, dst, send, recv, to_rank):
        return pltpu.make_async_remote_copy(src_ref=src, dst_ref=dst, send_sem=send, recv_sem=recv, device_id={'ep': to_rank}, device_id_type=MESH)

    shared = (su, sl, sd)
    hot = (hu, hl, hd)
    own = {'up': wsu, 'lin': wsl, 'dna': wsd.at[:, pl.ds(0, zh)], 'dnb': wsd.at[:, pl.ds(zh, zh)]}

    full = (wu.at[0], wl.at[0], wd.at[0])

    def half_of(n, c):
        return full[n].at[:, pl.ds(c * half, half)] if n < 2 else full[n].at[pl.ds(c * half, half), :]

    far = [remote(half_of(n, 1), hot[n], far_send.at[n], far_recv.at[n], 1) for n in range(3)]

    @pl.when(rank == 0)
    def _():
        for copy in far:
            copy.start()

    def ag_copy(n, step):
        name, axis, _ = SHARED[n]
        near, other = (x_chip, y_chip) if axis == 'x' else (y_chip, x_chip)
        src = region(shared, name, near) if step == 2 else own[name]
        dst = region(shared, name, near if step == 2 else chip)
        at = 4 * step + n
        return remote(src, dst, ag_send.at[at], ag_recv.at[at], (other if step else near) * 2 + core)

    def z_copy(n, step):
        name, axis, _ = SHARED[n]
        near, other = (x_chip, y_chip) if axis == 'x' else (y_chip, x_chip)
        at = region(shared, name, (near, other, xy_chip)[step])
        sem = 3 * n + step
        return pltpu.make_async_remote_copy(src_ref=at, dst_ref=at, send_sem=z_send.at[sem], recv_sem=z_recv.at[sem], device_id={'dp': 1 - row}, device_id_type=MESH)

    def in_row(n):
        return row == SHARED[n][2]

    for n in range(4):
        @pl.when(in_row(n))
        def _():
            ag_copy(n, 0).start()
            ag_copy(n, 1).start()
    local = [(wsu, small_a.at[0], region(shared, 'up', chip)), (wsl, small_a.at[1], region(shared, 'lin', chip)), (wsd, small_b, sd.at[pl.ds(pl.multiple_of(chip * part, 128), part), :])]
    loads = [pltpu.make_async_copy(src, mid, load_sem.at[n]) for n, (src, mid, _) in enumerate(local)]
    stores = [pltpu.make_async_copy(mid, dst, store_sem.at[n]) for n, (_, mid, dst) in enumerate(local)]
    mids = (big_a.at[0], big_a.at[1], big_b)
    own_loads = [pltpu.make_async_copy(half_of(n, 0), mids[n], load_sem.at[3 + n]) for n in range(3)]
    own_stores = [pltpu.make_async_copy(mids[n], hot[n], store_sem.at[3 + n]) for n in range(3)]
    for copy in loads:
        copy.start()

    @pl.when(rank == 0)
    def _():
        for copy in own_loads:
            copy.start()

    chunks = [(name, axis, slot, piece) for slot in range(4) for name, axis in PIECES for piece in range(2)]

    def hot_copy(n, to_chip, source):
        name, axis, slot, piece = chunks[n]
        return remote(strip(source, name, slot, piece), strip(hot, name, slot, piece), hot_send.at[n], hot_recv.at[n], to_chip * 2 + core)

    route = {'x': {0: 1, 1: 3, 3: 2}, 'y': {0: 2, 2: 3, 3: 1}}

    for n in range(4):
        @pl.when(in_row(n))
        def _():
            ag_copy(n, 0).wait_recv()
            ag_copy(n, 2).start()
            z_copy(n, 0).start()

    @pl.when(rank == 0)
    def _():
        lo = (full[0].at[:, pl.ds(0, half)], full[1].at[:, pl.ds(0, half)], full[2].at[pl.ds(0, half), :])
        for n, (name, axis, slot, piece) in enumerate(chunks):
            hot_copy(n, route[axis][0], lo).start()

    @pl.when(rank == 1)
    def _():
        for n in range(3):
            far[n].wait_recv()
        for n, (name, axis, slot, piece) in enumerate(chunks):
            hot_copy(n, route[axis][0], hot).start()

    for step in (1, 2):
        for n in range(4):
            @pl.when(in_row(n))
            def _():
                ag_copy(n, step).wait_recv()
                z_copy(n, step).start()
    for n in range(3):
        loads[n].wait()
        stores[n].start()

    @pl.when(rank == 0)
    def _():
        for n in range(3):
            own_loads[n].wait()
            own_stores[n].start()

    for me in (1, 2, 3):
        @pl.when(chip == me)
        def _():
            for n, (name, axis, slot, piece) in enumerate(chunks):
                if me in route[axis]:
                    hot_copy(n, 0, hot).wait_recv()
                    hot_copy(n, route[axis][me], hot).start()
            for n, (name, axis, slot, piece) in enumerate(chunks):
                if me not in route[axis]:
                    hot_copy(n, 0, hot).wait_recv()

    for me in (0, 1, 2, 3):
        @pl.when(chip == me)
        def _():
            for n, (name, axis, slot, piece) in enumerate(chunks):
                if me in route[axis]:
                    hot_copy(n, route[axis][me], hot).wait_send()

    for n in range(4):
        @pl.when(in_row(n))
        def _():
            for step in range(3):
                ag_copy(n, step).wait_send()
                z_copy(n, step).wait_send()

        @pl.when(jnp.logical_not(in_row(n)))
        def _():
            for step in range(3):
                z_copy(n, step).wait_recv()
    for copy in stores:
        copy.wait()

    @pl.when(rank == 0)
    def _():
        for n in range(3):
            far[n].wait_send()
            own_stores[n].wait()


def weights_call(ws_up, ws_lin, ws_down, w_up, w_lin, w_down):
    width, part = ws_up.shape
    half = 4 * part
    hbm = pl.BlockSpec(memory_space=pl.ANY)
    shapes = [jax.ShapeDtypeStruct(v, BF16) for v in ((width, half), (width, half), (half, width))]
    dma = pltpu.SemaphoreType.DMA
    return pl.pallas_call(
        functools.partial(weights_kernel, part),
        in_specs=[hbm] * 6,
        out_specs=[hbm] * 6,
        out_shape=shapes + shapes,
        scratch_shapes=[
            pltpu.VMEM((2, width, part), BF16), pltpu.VMEM((part, width), BF16), pltpu.VMEM((2, width, half), BF16), pltpu.VMEM((half, width), BF16),
            dma((6,)), dma((6,)), dma((3,)), dma((3,)), dma((12,)), dma((12,)), dma((12,)), dma((12,)), dma((32,)), dma((32,)),
        ],
        cost_estimate=pl.CostEstimate(flops=10 ** 11, bytes_accessed=5 * 10 ** 7, transcendentals=0),
        compiler_params=pltpu.CompilerParams(has_side_effects=True, vmem_limit_bytes=48 * 1024 * 1024),
    )(ws_up, ws_lin, ws_down, w_up, w_lin, w_down)


def place_kernel(plans, count, *refs):
    owner = lax.axis_index('ep') == 0
    zc = lax.axis_index('dp')
    sources, outs = refs[:count], refs[count + 3:count + 6]
    hold, in_sem, out_sem = refs[count + 6:]
    side = hold.shape[1]

    def pull(n):
        which, src, row, _, _, _ = plans[n]
        return pltpu.make_async_copy(sources[src].at[pl.ds(row, side)], hold.at[n], in_sem.at[n])

    def push(n):
        which, _, _, z_rel, slot, slot_dim = plans[n]
        zpos = (zc if z_rel == 0 else 1 - zc) * side
        where = (pl.ds(zpos, side), pl.ds(slot, side)) if slot_dim == 1 else (pl.ds(slot, side), pl.ds(pl.multiple_of(zpos, 128), side))
        return pltpu.make_async_copy(hold.at[n], outs[which].at[(0,) + where], out_sem.at[n])

    @pl.when(owner)
    def _():
        for n in range(len(plans)):
            pull(n).start()
        for n in range(len(plans)):
            pull(n).wait()
            push(n).start()
        for n in range(len(plans)):
            push(n).wait()


def place_call(states, norms, slot_dims, part):
    sources, plans, known = [], [], {}
    for which, (state, slot_dim) in enumerate(zip(states, slot_dims)):
        for (c, y, x, z), (array, row) in sorted(state.items()):
            if id(array) not in known:
                known[id(array)] = len(sources)
                sources.append(array)
            plans.append((which, known[id(array)], row, z, (c * 4 + y * 2 + x) * part, slot_dim))
    side = sources[0].shape[1]
    hbm = pl.BlockSpec(memory_space=pl.ANY)
    return pl.pallas_call(
        functools.partial(place_kernel, tuple(plans), len(sources)),
        in_specs=[hbm] * (len(sources) + 3),
        out_specs=[hbm] * 3,
        out_shape=[jax.ShapeDtypeStruct(v.shape, v.dtype) for v in norms],
        scratch_shapes=[pltpu.VMEM((len(plans), side, side), F32), pltpu.SemaphoreType.DMA((len(plans),)), pltpu.SemaphoreType.DMA((len(plans),))],
        input_output_aliases={len(sources) + k: k for k in range(3)},
        cost_estimate=pl.CostEstimate(flops=2 * 10 ** 10, bytes_accessed=57 * 10 ** 6, transcendentals=0),
        compiler_params=pltpu.CompilerParams(vmem_limit_bytes=48 * 1024 * 1024),
    )(*sources, *norms)


def solution(mesh):
    dp_size, ep_size = mesh.shape['dp'], mesh.shape['ep']
    total = dp_size * ep_size
    both = ('dp', 'ep')

    def swap(value, axis):
        bit = ep_size if axis == 'z' else BIT[axis]
        return lax.ppermute(value, both, [(i, i ^ bit) for i in range(total)])

    def move(value, pairs):
        return lax.ppermute(value, both, [(z * ep_size + s, z * ep_size + d) for z in range(dp_size) for s, d in pairs])

    def local_step(hidden, route_idx, gates, grad_out, w_up, w_lin, w_down, ws_up, ws_lin, ws_down):
        tok, width = hidden.shape
        ff = w_up.shape[2]
        part = ff // ep_size
        half = ff // 2
        zh = width // 2
        cap = (tok + ep_size - 2) // (ep_size - 1)
        cap = (cap + 7) // 8 * 8
        rank = lax.axis_index('ep')
        zc = lax.axis_index('dp')
        core0 = rank % 2 == 0
        x0 = (rank // 2) % 2 == 0
        y0 = rank // 4 == 0
        is_owner = rank == 0

        s_up, s_lin, s_dn, h_up, h_lin, h_dn = weights_call(ws_up, ws_lin, ws_down, w_up, w_lin, w_down)
        route_idx, gates, hidden, grad_out = lax.optimization_barrier((route_idx, gates, hidden, grad_out, s_up))[:4]

        ids = route_idx.reshape(-1)
        is_hot = ids == HOT
        gate = gates.astype(F32)
        d_tok = (gate * grad_out.astype(F32)).astype(BF16)
        d_hot = jnp.where(is_hot[:, None], d_tok, jnp.zeros_like(d_tok))
        onehot = (ids[:, None] == jnp.arange(ep_size)[None, :]).astype(jnp.int32)
        before = jnp.cumsum(onehot, axis=0) - onehot
        pos_in = jnp.sum(before * onehot, axis=1)
        slots = ep_size * cap
        dest = jnp.where(is_hot, slots, ids * cap + pos_in)
        src_map = jnp.zeros((slots,), jnp.int32).at[dest].set(jnp.arange(tok, dtype=jnp.int32) + 1, mode='drop')

        pair = lambda rows: jnp.concatenate([rows, swap(rows, 'c')], axis=0)
        x2, dy2, dh2 = pair(hidden), pair(grad_out), pair(d_hot)

        def after(values, token):
            return lax.optimization_barrier((values, token))[0]

        def join(own, partner):
            return own + swap(partner, 'c')

        def local_rows(d_rows, up_w, lin_w, dn_w):
            return expert_call(x2, d_rows, (0, 0), up_w, lin_w, dn_w, F32, 512, 2 * tok, 2)

        def local_grads(rows, d_rows, saved):
            act, d_up, d_lin = saved[:3]
            return [mm(rows, d_up, 0, 0), mm(rows, d_lin, 0, 0), mm(act, d_rows, 0, 0)]

        SLOT_DIMS = (1, 1, 0)
        ORDERS = ('xyz', 'yzx', 'zxy')

        def split(grad, slot_dim, axis, slots_here):
            cut = lambda v, k: lax.slice_in_dim(v, k * part, (k + 1) * part, axis=slot_dim)
            if axis == 'z':
                take = lambda k: lax.dynamic_slice_in_dim(grad, k * zh, zh, axis=1 - slot_dim)
                return take(1 - zc), take(zc), slots_here
            bit = 1 if axis == 'x' else 2
            low = [k for k, q in enumerate(slots_here) if not q & bit]
            high = [k for k, q in enumerate(slots_here) if q & bit]
            low_cut = jnp.concatenate([cut(grad, k) for k in low], axis=slot_dim)
            high_cut = jnp.concatenate([cut(grad, k) for k in high], axis=slot_dim)
            lower = x0 if axis == 'x' else y0
            return jnp.where(lower, high_cut, low_cut), jnp.where(lower, low_cut, high_cut), [slots_here[k] for k in low]

        class Reduction:
            def __init__(self, grads):
                self.now, self.slots, self.step = list(grads), [[0, 1, 2, 3]] * 3, 0

            def start(self):
                self.keep, self.got = [None] * 3, [None] * 3
                for n in range(3):
                    axis = ORDERS[n][self.step]
                    send, self.keep[n], self.slots[n] = split(self.now[n], SLOT_DIMS[n], axis, self.slots[n])
                    self.got[n] = swap(send, axis)
                self.step += 1

            def finish(self, token):
                self.got = after(self.got, token)
                self.now = [keep + got for keep, got in zip(self.keep, self.got)]

        EVEN = [0, 2, 4, 6]

        class ToOwner:
            def __init__(self, blocks):
                self.live, self.step = [EVEN] * 3, 0
                self.have = [[block, move(block, [(r + 1, r) for r in EVEN])] for block in blocks]
                self.keys = [[(0, 0, 0, 0), (1, 0, 0, 0)] for _ in blocks]

            def start(self):
                for n in range(3):
                    axis, live = ('zyx', 'xzy', 'yxz')[n][self.step], self.live[n]
                    packed = jnp.concatenate(self.have[n], axis=0)
                    if axis == 'z':
                        got = lax.ppermute(packed, both, [(z * ep_size + r, (1 - z) * ep_size + r) for z in range(dp_size) for r in live])
                    else:
                        got = move(packed, [(r, r - BIT[axis]) for r in live if r & BIT[axis]])
                        self.live[n] = [r for r in live if not r & BIT[axis]]
                    dim = {'y': 1, 'x': 2, 'z': 3}[axis]
                    self.have[n] = [packed, got]
                    self.keys[n] = self.keys[n] + [k[:dim] + (1,) + k[dim + 1:] for k in self.keys[n]]
                self.step += 1

            def finish(self, token):
                got = after([h[1] for h in self.have], token)
                self.have = [[h[0], g] for h, g in zip(self.have, got)]

            def blocks(self):
                out = []
                for have, keys in zip(self.have, self.keys):
                    rows = have[0].shape[0] // zh
                    out.append({k: (have[m // rows], m % rows * zh) for m, k in enumerate(keys)})
                return out

        rows = jnp.take(jnp.concatenate([hidden, d_tok], axis=1), jnp.maximum(src_map - 1, 0), axis=0)
        rows = rows * (src_map > 0).astype(BF16)[:, None]
        mine = lax.all_to_all(rows.reshape(ep_size, cap, 2 * width), 'ep', 0, 0, tiled=True).reshape(slots, 2 * width)
        far = swap(mine, 'z')
        tile = slots // 2

        dh2 = after(dh2, mine)
        h_rows = local_rows(dh2, h_up, h_lin, h_dn)
        h_grads = local_grads(x2, dh2, h_rows)
        h_sum = Reduction(h_grads)
        h_sum.start()

        dy2 = after(dy2, h_grads)
        s_rows = local_rows(dy2, s_up, s_lin, s_dn)
        h_sum.finish(s_rows[0])
        h_sum.start()

        s_x2, s_act = after((x2, s_rows[0]), h_sum.keep)
        s_grads = local_grads(s_x2, dy2, [s_act] + list(s_rows[1:3]))
        h_sum.finish(s_grads)
        h_sum.start()

        def z_join(block, dim):
            got = swap(block, 'z')
            return jnp.where(zc == 0, jnp.concatenate([block, got], axis=dim), jnp.concatenate([got, block], axis=dim))

        s_sum = Reduction(after(s_grads, h_sum.keep))
        s_sum.start()

        mine = after(mine, s_sum.keep)
        *saved, n_out, n_dx = expert_call(mine, mine, (0, 1), w_up[0], w_lin[0], w_down[0], BF16, tile, 2 * slots)
        h_sum.finish(saved[0])
        owner = ToOwner(h_sum.now)
        owner.start()
        s_sum.finish(saved[0])
        s_sum.start()
        back = jnp.concatenate([n_out, n_dx], axis=1).reshape(ep_size, cap, 2 * width)
        back = lax.all_to_all(back, 'ep', 0, 0, tiled=True).reshape(slots, 2 * width)

        far = after(far, (saved[0], s_sum.keep))
        saved = expert_call(far, far, (0, 1), w_up[0], w_lin[0], w_down[0], BF16, tile, 2 * slots, 1, tuple(saved))
        owner.finish(saved[0])
        owner.start()
        s_sum.finish(saved[0])
        s_sum.start()

        n_rows = jnp.concatenate([mine, far], axis=0)
        n_x, n_d = after((n_rows[:, :width], n_rows[:, width:]), s_sum.keep)
        g_up = mm(n_x, saved[1], 0, 0)
        owner.finish(g_up)
        owner.start()
        s_sum.finish(g_up)
        dws = [z_join(s_sum.now[0], 0), z_join(s_sum.now[1], 0), z_join(s_sum.now[2], 1)]
        n_x, n_d = after((n_x, n_d), owner.have[0][0])
        n_grads = [g_up, mm(n_x, saved[2], 0, 0), mm(saved[0], n_d, 0, 0)]
        owner.finish(n_grads)
        dw = place_call(owner.blocks(), [g[None] for g in n_grads], SLOT_DIMS, part)

        h_out, h_dx = join(*h_rows[3:5]), join(*h_rows[5:7])
        s_out, s_dx = join(*s_rows[3:5]), join(*s_rows[5:7])
        back = jnp.take(back, jnp.minimum(dest, slots - 1), axis=0)

        hot_row = is_hot[:, None]
        rounded = lambda v: lax.reduce_precision(v, exponent_bits=8, mantissa_bits=7)
        o_tok = jnp.where(hot_row, rounded(h_out), back[:, :width].astype(F32))
        p_tok = jnp.where(hot_row, rounded(h_dx), back[:, width:].astype(F32))
        y_tok = (gate * o_tok + s_out).astype(BF16)
        d_hidden = (p_tok + s_dx).astype(BF16)
        return (y_tok, d_hidden, dw[0], dw[1], dw[2], dws[0], dws[1], dws[2])

    tok_spec = P(both, None)
    expert_spec = P('ep', None, None)
    col_spec = P(None, 'ep')
    row_spec = P('ep', None)
    return jax.shard_map(local_step, mesh=mesh, in_specs=(tok_spec, tok_spec, tok_spec, tok_spec, expert_spec, expert_spec, expert_spec, col_spec, col_spec, row_spec), out_specs=(tok_spec, tok_spec, expert_spec, expert_spec, expert_spec, col_spec, col_spec, row_spec), check_vma=False)
```
